128 devices in a mesh: wide: 8 (over y_lo, z), narrow: 16 (over y_hi, x, core).
Axes of the slice: x: 4, y: 4 (y_hi: 2, y_lo: 2; y = y_hi * 2 + y_lo), z: 4, core: 2. Of those that a mesh axis runs over, the one named last changes fastest.
Arguments:
- saved_inputs: bfloat16 [2048, 5120], P('wide', 'narrow'), may hold values from -6 to 6
- out_grads: bfloat16 [2048, 5120], P('wide', 'narrow'), may hold values from -48 to 48
- seq_ids: int32 [2048], P('wide'), may hold values from 0 to 15, as said below
- seq_counts: int32 [16], P('wide'), may hold values from 64 to 192, as said below
- basis_in: bfloat16 [5120, 5120], P('narrow'), may hold values from -0.078125 to 0.078125
- basis_out: bfloat16 [5120, 5120], P('narrow'), may hold values from -0.078125 to 0.078125
- query_rotated: bfloat16 [5120, 5120], P('narrow', 'wide'), may hold values from -6 to 6
- damping: float32 [], replicated, may hold values from 0.05 to 0.5
Outputs:
- eigenvalues: float32 [5120, 5120], P('narrow', 'wide')
- preconditioned: float32 [5120, 5120], P('narrow', 'wide')
The draws below stay inside these ranges and needn't reach their ends.
Inputs may be any that keep to these rules, and one draw needn't show every extreme that they name: seq_ids names for each token its sequence; the 256 tokens of block w of the token axis belong to the sequences 2 * w to 2 * w + 1, each having at least one token. seq_counts[s] is the number of tokens whose seq_ids equal s.
All inputs are finite; a program needn't handle non-finite values.
Results may differ from the reference program's by a relative error of at most 0.01.
Values may be sent and summed in bfloat16 or wider, within the bound.
A program may use at most 128 MiB of HBM per device.

```python
import math
import jax
import jax.numpy as jnp
from jax import lax

D = 5120
TOK_DEV = 256
SEQ_DEV = 2
MAXLEN = 192
TOKENS = 2048
SEQS = 16


def first_lengths(key):
    groups = SEQS // SEQ_DEV
    len_key, pick_key = jax.random.split(jax.random.fold_in(key, 7))
    first_len = jax.random.randint(len_key, (groups,), TOK_DEV - MAXLEN, MAXLEN + 1)
    chosen = jax.random.randint(pick_key, (), 0, groups)
    return jnp.where(jnp.arange(groups) == chosen, MAXLEN, first_len).astype(jnp.int32)


def draw_seq_counts(key, part):
    first_len = first_lengths(key)
    return jnp.stack([first_len, TOK_DEV - first_len], axis=1).reshape(-1).astype(jnp.int32)


def draw_seq_ids(key, part):
    first_len = first_lengths(key)
    groups = first_len.shape[0]
    position = jnp.arange(TOK_DEV, dtype=jnp.int32)[None, :]
    within = jnp.where(position < first_len[:, None], 0, 1).astype(jnp.int32)
    return (within + SEQ_DEV * jnp.arange(groups, dtype=jnp.int32)[:, None]).reshape(-1).astype(jnp.int32)


def block_levels(own_key, shape, shards, smallest, largest):
    factor_of, own = 1.0, jax.random.fold_in(own_key, 6)
    for axis_at, blocks in shards:
        steps = jnp.exp(jax.random.uniform(jax.random.fold_in(own, axis_at), (blocks,), jnp.float32, smallest / len(shards), largest / len(shards)))
        factor_of = factor_of * jnp.repeat(steps, shape[axis_at] // blocks).reshape([-1 if axis == axis_at else 1 for axis in range(len(shape))])
    return factor_of


def gaussian(own_key, shape, scale, limit, pieces=(), held_as=jnp.bfloat16):
    array = jax.random.normal(own_key, shape, jnp.float32) * scale
    if len(pieces) > 0:
        array = block_levels(own_key, shape, pieces, -0.22, 0.18) * array
    return jnp.clip(array, min=-limit, max=limit).astype(held_as)


def setup_inputs(seed: int = 0) -> dict:
    streams_of = jax.random.split(jax.random.key(seed), 9)
    return {
        "saved_inputs": gaussian(streams_of[0], (TOKENS, D), 1.0, 6.0, ((0, 8), (1, 16))),
        "out_grads": gaussian(streams_of[1], (TOKENS, D), 8.0, 48.0, ((0, 8), (1, 16))),
        "seq_ids": draw_seq_ids(jax.random.fold_in(streams_of[8], 71), 0),
        "seq_counts": draw_seq_counts(jax.random.fold_in(streams_of[8], 71), 0),
        "basis_in": gaussian(streams_of[4], (D, D), D ** -0.5, 0.078125, ((0, 16),)),
        "basis_out": gaussian(streams_of[5], (D, D), D ** -0.5, 0.078125, ((0, 16),)),
        "query_rotated": gaussian(streams_of[6], (D, D), 1.0, 6.0, ((0, 16), (1, 8))),
        "damping": jnp.clip(jnp.exp(jax.random.uniform(streams_of[7], (), jnp.float32, math.log(0.05), math.log(0.5))), 0.05, 0.5),
    }


def reference(saved_inputs, out_grads, seq_ids, seq_counts, basis_in, basis_out, query_rotated, damping):
    rot_in = jnp.dot(saved_inputs, basis_in, preferred_element_type=jnp.float32).astype(jnp.bfloat16)
    rot_grad = jnp.dot(out_grads, basis_out, preferred_element_type=jnp.float32).astype(jnp.bfloat16)

    def add_sequence(seq_index, running):
        seq_index = seq_index.astype(jnp.int32)
        group_start = (seq_index // SEQ_DEV) * TOK_DEV
        rows_in = lax.dynamic_slice_in_dim(rot_in, group_start, TOK_DEV, 0)
        rows_grad = lax.dynamic_slice_in_dim(rot_grad, group_start, TOK_DEV, 0)
        seq_here = lax.dynamic_slice_in_dim(seq_ids, group_start, TOK_DEV, 0)
        count = lax.dynamic_slice_in_dim(seq_counts, seq_index, 1, 0)[0].astype(jnp.float32)
        weight = jnp.where(seq_here == seq_index, 1.0, 0.0).astype(jnp.float32) / count
        weighted = (rows_grad.astype(jnp.float32) * weight[:, None]).astype(jnp.bfloat16)
        per_seq = lax.dot_general(weighted, rows_in, (((0,), (0,)), ((), ())), preferred_element_type=jnp.float32)
        return running + per_seq * per_seq

    empty = jnp.zeros((D, D), jnp.float32)
    eigenvalues = lax.fori_loop(0, SEQS, add_sequence, empty) / SEQS
    scaled = (query_rotated.astype(jnp.float32) / (eigenvalues + damping)).astype(jnp.bfloat16)
    middle = jnp.dot(basis_out, scaled, preferred_element_type=jnp.float32).astype(jnp.bfloat16)
    preconditioned = lax.dot_general(middle, basis_in, (((1,), (1,)), ((), ())), preferred_element_type=jnp.float32)
    return eigenvalues, preconditioned
```

```python
import jax
import jax.numpy as jnp
from jax import lax
from jax.experimental import pallas as pl
from jax.experimental.pallas import tpu as pltpu
from jax.sharding import PartitionSpec as P

MESH = pl.DeviceIdType.MESH
BF = jnp.bfloat16
F32 = jnp.float32

D = 5120
TOK = 256
NB = 320
WB = 640
SUB = 16
GROWS = NB + 16
NSEM = 192


def kernel(
    x_ref, g_ref, ids_ref, cnt_ref, damp_ref, q_ref, bin_hbm, bout_hbm,
    eig_ref, out_ref,
    bout, incols, xw, pt, ps, rh, rf, ry, ryb, gt, rot, rotacc, sall, acc, mid, pb, eh, ef, ey, eyb,
    ssem, rsem, lsem,
):
    w = lax.axis_index("wide")
    n = lax.axis_index("narrow")
    yl, z = w // 4, w % 4
    yh, x, k = n // 8, (n // 2) % 4, n % 2

    def nslot(dx, dy):
        return (yh + dy) % 2 * 8 + (x + dx) % 4 * 2 + k

    def wslot(dz, dy):
        return (yl + dy) % 2 * 4 + (z + dz) % 4

    def cslot(dx, dy):
        return (yh + dy) % 2 * 4 + (x + dx) % 4

    sib = (w, n + 1 - 2 * k)
    xr, xl, yp = (w, nslot(1, 0)), (w, nslot(3, 0)), (w, nslot(0, 1))
    zr, zl, yq = (wslot(1, 0), n), (wslot(3, 0), n), (wslot(0, 1), n)
    ynb = (wslot(0, 1), nslot(0, 1))

    count = [0]
    sent = []

    def send(src, dst, to):
        c = count[0]
        count[0] += 1
        copy = pltpu.make_async_remote_copy(
            src_ref=src, dst_ref=dst, send_sem=ssem.at[c], recv_sem=rsem.at[c],
            device_id=to, device_id_type=MESH,
        )
        copy.start()
        sent.append(copy)
        return copy

    load_bout = pltpu.make_async_copy(bout_hbm, bout, lsem.at[0])
    load_bout.start()
    mine = pl.ds(pl.multiple_of(w * WB, 128), WB)
    load_cols = pltpu.make_async_copy(bin_hbm.at[:, mine], incols.at[n], lsem.at[1])
    load_cols.start()

    barrier = pltpu.get_barrier_semaphore()
    others = [(w, (n + d) % 16) for d in range(1, 16)]
    for to in others + [zr, zl, yq, ynb]:
        pl.semaphore_signal(barrier, inc=1, device_id=to, device_id_type=MESH)
    pl.semaphore_wait(barrier, len(others) + 4)

    class Gather:
        def __init__(self, view, half, slot, right, left, part, to_sib):
            self.view, self.half, self.slot = view, half, slot
            self.right, self.left, self.part, self.to_sib = right, left, part, to_sib
            self.sibs = []

        def fwd(self, dx, dy):
            if self.to_sib:
                v = self.view(self.slot(dx, dy))
                self.sibs.append(send(v, v, sib))

        def hop(self, v, to):
            return send(v, v, to)

        def start(self, src=None, part_src=None):
            v = self.view(self.slot(0, 0))
            src = v if src is None else src
            self.r = send(src, v, self.right)
            self.l = send(src, v, self.left)
            self.p = send(src if part_src is None else part_src, v, self.part)
            if self.to_sib:
                self.sibs.append(send(src, v, sib))

        def near(self):
            self.r.wait_recv()
            self.fr = self.hop(self.half(self.slot(3, 0), 0), self.right)
            self.fwd(3, 0)
            self.l.wait_recv()
            self.fl = self.hop(self.half(self.slot(1, 0), 1), self.left)
            self.fwd(1, 0)

        def across(self):
            self.p.wait_recv()
            v = self.view(self.slot(0, 1))
            self.pr = self.hop(v, self.right)
            self.pl = self.hop(v, self.left)
            self.fwd(0, 1)

        def far(self):
            self.fr.wait_recv()
            self.fl.wait_recv()
            self.fwd(2, 0)

        def across_near(self):
            self.pr.wait_recv()
            self.pfr = self.hop(self.half(self.slot(3, 1), 0), self.right)
            self.fwd(3, 1)
            self.pl.wait_recv()
            self.pfl = self.hop(self.half(self.slot(1, 1), 1), self.left)
            self.fwd(1, 1)

        def across_far(self):
            self.pfr.wait_recv()
            self.pfl.wait_recv()
            self.fwd(2, 1)

        def got_sib(self, i):
            self.sibs[i].wait_recv()

    class Scatter:
        def __init__(self, view, half, slot, right, left, part, h, f, fy, fyb):
            self.view, self.half, self.slot = view, half, slot
            self.right, self.left, self.part = right, left, part
            self.h, self.f, self.fy, self.fyb = h, f, fy, fyb
            self.one, self.two = {}, {}

        def first(self, y):
            c = self.slot(2, y)
            self.one[y] = (
                send(self.half(c, 1), self.h.at[y, 0], self.right),
                send(self.half(c, 0), self.h.at[y, 1], self.left),
            )

        def second(self, y):
            for d, (dx, part, to) in enumerate(((1, 1, self.right), (3, 0, self.left))):
                self.one[y][d].wait_recv()
                v = self.half(self.slot(dx, y), part)
                v[...] = (v[...].astype(F32) + self.h[y, d].astype(F32)).astype(BF)
                copy = send(self.view(self.slot(dx, y)), self.f.at[y, d], to)
                self.two[y] = self.two.get(y, ()) + (copy,)

        def total(self, y):
            for copy in self.two[y]:
                copy.wait_recv()
            own = self.view(self.slot(0, y))
            return own[...].astype(F32) + self.f[y, 0].astype(F32) + self.f[y, 1].astype(F32)

        def third(self):
            self.fyb[...] = self.total(1).astype(BF)
            self.last = send(self.fyb, self.fy, self.part)

        def fourth(self):
            t = self.total(0)
            self.last.wait_recv()
            return t + self.fy[...].astype(F32)

    theirs = pl.ds(pl.multiple_of(wslot(0, 1) * WB, 128), WB)
    cols = Gather(
        lambda s: incols.at[s], lambda s, h: incols.at[s, pl.ds(160 * h, 160)],
        nslot, xr, xl, ynb, True,
    )
    cols.start(bin_hbm.at[:, mine], bin_hbm.at[:, theirs])

    put_x = []
    for to in others:
        rows = pl.ds(pl.multiple_of(to[1] * SUB, SUB), SUB)
        put_x.append(send(x_ref.at[rows], xw.at[w, n], to))
    xw[w, n] = x_ref[pl.ds(pl.multiple_of(n * SUB, SUB), SUB), :]

    load_bout.wait()

    def rotate_grad(c, _):
        at = pl.ds(pl.multiple_of(c * WB, 128), WB)
        part = jnp.dot(g_ref[...], bout[:, at], preferred_element_type=F32).T
        pt[0, c] = part[:NB].astype(BF)
        pt[1, c] = part[NB:].astype(BF)
        return _

    lax.fori_loop(0, 8, rotate_grad, 0)
    swap = send(pt.at[1 - k], ps, sib)

    for copy in put_x:
        copy.wait_recv()
    xg = Gather(
        lambda s: xw.at[s], lambda s, h: xw.at[s, pl.ds(8 * h, 8)], wslot, zr, zl, yq, False
    )
    xg.start()

    swap.wait_recv()
    grads = Scatter(
        lambda c: ps.at[c], lambda c, h: ps.at[c, pl.ds(160 * h, 160)],
        cslot, xr, xl, yp, rh, rf, ry, ryb,
    )

    def both(dx, dy):
        c = cslot(dx, dy)
        ps[c] = (ps[c].astype(F32) + pt[k, c].astype(F32)).astype(BF)

    both(2, 1)
    grads.first(1)
    both(2, 0)
    grads.first(0)
    for dy in (1, 0):
        for dx in (1, 3, 0):
            both(dx, dy)

    cols.near()
    xg.near()
    xg.across()
    grads.second(1)
    grads.second(0)
    cols.across()
    xg.far()
    xg.across_near()
    grads.third()
    xg.across_far()
    load_cols.wait()

    def rotate_in(dx, dy, first=False):
        total = None
        for core in range(2):
            s = cslot(dx, dy) * 2 + core
            part = jnp.dot(
                xw[:, s].reshape(8 * SUB, NB), incols[s], preferred_element_type=F32
            )
            total = part if total is None else total + part
        rotacc[...] = total if first else rotacc[...] + total

    cols.got_sib(0)
    rotate_in(0, 0, True)
    cols.far()
    rotg = grads.fourth()

    is_first = ids_ref[...] == 2 * w
    count_of = jnp.where(
        is_first, jnp.broadcast_to(cnt_ref[:, 0:1], (1, TOK)), jnp.broadcast_to(cnt_ref[:, 1:2], (1, TOK))
    )
    weight = 1.0 / count_of.astype(F32)
    gt[w, :NB] = (rotg.astype(BF).astype(F32) * weight).astype(BF)
    gt[w, NB:] = jnp.broadcast_to(jnp.where(is_first, 1.0, 0.0).astype(BF), (16, TOK))
    gg = Gather(
        lambda s: gt.at[s],
        lambda s, h: gt.at[s, pl.ds(176 * h, 176 - 16 * h)],
        wslot, zr, zl, yq, False,
    )
    gg.start()

    cols.got_sib(1)
    rotate_in(3, 0)
    cols.got_sib(2)
    rotate_in(1, 0)
    cols.across_near()
    cols.got_sib(3)
    rotate_in(0, 1)
    cols.got_sib(4)
    rotate_in(2, 0)
    gg.near()
    cols.got_sib(5)
    rotate_in(3, 1)
    cols.got_sib(6)
    rotate_in(1, 1)
    cols.across_far()
    cols.got_sib(7)
    rotate_in(2, 1)

    rot[:, pl.ds(pl.multiple_of(n * SUB, SUB), SUB), :] = (
        rotacc[...].astype(BF).reshape(8, SUB, WB)
    )

    def rows_of(s):
        return pl.ds(pl.multiple_of(s * SUB, SUB), SUB)

    rg = Gather(
        lambda s: rot.at[:, rows_of(s)],
        lambda s, h: rot.at[pl.ds(4 * h, 4), rows_of(s)],
        nslot, xr, xl, yp, True,
    )
    rg.start()
    gg.across()
    rg.near()
    rg.across()
    gg.far()
    gg.across_near()
    rg.far()
    rg.across_near()
    gg.across_far()
    rg.across_far()
    for i in range(8):
        rg.got_sib(i)

    acc[...] = jnp.zeros_like(acc)

    def fit(b, _):
        grad = gt[b, :NB]
        mask = gt[b, NB:NB + 1]
        one = grad * mask
        rows = rot[b]
        p = jnp.dot(one, rows, preferred_element_type=F32)
        r = jnp.dot(grad - one, rows, preferred_element_type=F32)
        acc[...] += p * p + r * r
        return _

    lax.fori_loop(0, 8, fit, 0)
    eig = acc[...] * (1.0 / 16)
    eig_ref[...] = eig
    sall[n] = (q_ref[...].astype(F32) / (eig + damp_ref[...])).astype(BF)

    sg = Gather(
        lambda s: sall.at[s], lambda s, h: sall.at[s, pl.ds(160 * h, 160)],
        nslot, xr, xl, yp, True,
    )
    sg.start()

    def rotate_out(dx, dy, first=False):
        c = cslot(dx, dy)
        at = pl.ds(pl.multiple_of(c * WB, 128), WB)
        part = jnp.dot(
            bout[:, at], sall[pl.ds(2 * c, 2)].reshape(WB, WB), preferred_element_type=F32
        )
        acc[...] = part if first else acc[...] + part

    sg.got_sib(0)
    rotate_out(0, 0, True)
    sg.near()
    sg.got_sib(1)
    rotate_out(3, 0)
    sg.got_sib(2)
    rotate_out(1, 0)
    sg.across()
    sg.far()
    sg.got_sib(3)
    rotate_out(0, 1)
    sg.got_sib(4)
    rotate_out(2, 0)
    sg.across_near()
    sg.got_sib(5)
    rotate_out(3, 1)
    sg.got_sib(6)
    rotate_out(1, 1)
    sg.across_far()
    sg.got_sib(7)
    rotate_out(2, 1)
    mid[...] = acc[...].astype(BF)

    def back(dz, dy):
        s = wslot(dz, dy)
        pb[s] = lax.dot_general(
            mid[...], incols[pl.ds(2 * s, 2)].reshape(WB, WB), (((1,), (1,)), ((), ())),
            preferred_element_type=F32,
        ).astype(BF)

    es = Scatter(
        lambda s: pb.at[s], lambda s, h: pb.at[s, pl.ds(160 * h, 160)],
        wslot, zr, zl, yq, eh, ef, ey, eyb,
    )
    back(2, 1)
    es.first(1)
    back(2, 0)
    es.first(0)
    for dy in (1, 0):
        for dz in (1, 3, 0):
            back(dz, dy)
    es.second(1)
    es.second(0)
    es.third()
    out_ref[...] = es.fourth()

    for copy in sent:
        copy.wait_send()


def shards(
    saved_inputs, out_grads, seq_ids, seq_counts, basis_in, basis_out, query_rotated, damping
):
    vm = pl.BlockSpec(memory_space=pltpu.VMEM)
    hbm = pl.BlockSpec(memory_space=pl.ANY)
    tile = jax.ShapeDtypeStruct((NB, WB), F32)
    return pl.pallas_call(
        kernel,
        out_shape=(tile, tile),
        in_specs=[vm] * 6 + [hbm] * 2,
        out_specs=(vm, vm),
        scratch_shapes=[
            pltpu.VMEM((NB, D), BF),
            pltpu.VMEM((16, NB, WB), BF),
            pltpu.VMEM((8, 16, SUB, NB), BF),
            pltpu.VMEM((2, 8, NB, TOK), BF),
            pltpu.VMEM((8, NB, TOK), BF),
            pltpu.VMEM((2, 2, NB // 2, TOK), BF),
            pltpu.VMEM((2, 2, NB, TOK), BF),
            pltpu.VMEM((NB, TOK), BF),
            pltpu.VMEM((NB, TOK), BF),
            pltpu.VMEM((8, GROWS, TOK), BF),
            pltpu.VMEM((8, TOK, WB), BF),
            pltpu.VMEM((8 * SUB, WB), F32),
            pltpu.VMEM((16, NB, WB), BF),
            pltpu.VMEM((NB, WB), F32),
            pltpu.VMEM((NB, WB), BF),
            pltpu.VMEM((8, NB, WB), BF),
            pltpu.VMEM((2, 2, NB // 2, WB), BF),
            pltpu.VMEM((2, 2, NB, WB), BF),
            pltpu.VMEM((NB, WB), BF),
            pltpu.VMEM((NB, WB), BF),
            pltpu.SemaphoreType.DMA((NSEM,)),
            pltpu.SemaphoreType.DMA((NSEM,)),
            pltpu.SemaphoreType.DMA((2,)),
        ],
        compiler_params=pltpu.CompilerParams(
            collective_id=0, has_side_effects=True, vmem_limit_bytes=60 * 1024 * 1024
        ),
    )(
        saved_inputs, out_grads, seq_ids.reshape(1, -1), seq_counts.reshape(1, -1),
        damping.reshape(1, 1), query_rotated, basis_in, basis_out,
    )


def solution(mesh):
    return jax.shard_map(
        shards,
        mesh=mesh,
        in_specs=(
            P("wide", "narrow"),
            P("wide", "narrow"),
            P("wide"),
            P("wide"),
            P("narrow", None),
            P("narrow", None),
            P("narrow", "wide"),
            P(),
        ),
        out_specs=(P("narrow", "wide"), P("narrow", "wide")),
        check_vma=False,
    )
```

```python
import jax
import jax.numpy as jnp
from jax import lax
from jax.experimental import pallas as pl
from jax.experimental.pallas import tpu as pltpu
from jax.sharding import PartitionSpec as P

MESH = pl.DeviceIdType.MESH
BF = jnp.bfloat16
F32 = jnp.float32

D = 5120
TOK = 256
NB = 320
WB = 640
SUB = 16
GROWS = NB + 16
PARTS = ((0, 256), (256, 256), (512, 128))
NSEM = 256


def kernel(
    ids_ref, cnt_ref, damp_ref, x_hbm, g_hbm, q_hbm, bin_hbm, bout_hbm,
    eig_hbm, out_hbm,
    xt, gtt, xv, gv, qv, bout, incols, xw, pt, ps, rh, rf, ry, ryb, gt, rot, rotacc, tall, acc, out,
    scaled, pb, eh, ef, ey, eyb,
    ssem, rsem, lsem,
):
    w = lax.axis_index("wide")
    n = lax.axis_index("narrow")
    yl, z = w // 4, w % 4
    yh, x, k = n // 8, (n // 2) % 4, n % 2

    def nslot(dx, dy):
        return (yh + dy) % 2 * 8 + (x + dx) % 4 * 2 + k

    def wslot(dz, dy):
        return (yl + dy) % 2 * 4 + (z + dz) % 4

    def cslot(dx, dy):
        return (yh + dy) % 2 * 4 + (x + dx) % 4

    sib = (w, n + 1 - 2 * k)
    xr, xl, yp = (w, nslot(1, 0)), (w, nslot(3, 0)), (w, nslot(0, 1))
    zr, zl, yq = (wslot(1, 0), n), (wslot(3, 0), n), (wslot(0, 1), n)
    ynb = (wslot(0, 1), nslot(0, 1))

    count = [0]
    sent = []

    def send(src, dst, to):
        c = count[0]
        count[0] += 1
        copy = pltpu.make_async_remote_copy(
            src_ref=src, dst_ref=dst, send_sem=ssem.at[c], recv_sem=rsem.at[c],
            device_id=to, device_id_type=MESH,
        )
        copy.start()
        sent.append(copy)
        return copy

    load_x = pltpu.make_async_copy(x_hbm, xt, lsem.at[2])
    load_x.start()
    load_g = pltpu.make_async_copy(g_hbm, gtt, lsem.at[3])
    load_g.start()
    load_q = pltpu.make_async_copy(q_hbm, qv, lsem.at[4])
    load_bout = pltpu.make_async_copy(bout_hbm, bout, lsem.at[0])
    load_bout.start()
    mine = pl.ds(pl.multiple_of(w * WB, 128), WB)
    load_cols = pltpu.make_async_copy(bin_hbm.at[:, mine], incols.at[n], lsem.at[1])
    load_cols.start()
    load_q.start()

    barrier = pltpu.get_barrier_semaphore()
    others = [(w, (n + d) % 16) for d in range(1, 16)]
    for to in others + [zr, zl, yq, ynb]:
        pl.semaphore_signal(barrier, inc=1, device_id=to, device_id_type=MESH)
    load_x.wait()
    xv[...] = xt[...].astype(F32).T.astype(BF)
    load_g.wait()
    gv[...] = gtt[...].astype(F32).T.astype(BF)
    pl.semaphore_wait(barrier, len(others) + 4)

    class Gather:
        def __init__(self, view, half, slot, right, left, part, to_sib):
            self.view, self.half, self.slot = view, half, slot
            self.right, self.left, self.part, self.to_sib = right, left, part, to_sib
            self.sibs = []

        def fwd(self, dx, dy):
            if self.to_sib:
                v = self.view(self.slot(dx, dy))
                self.sibs.append(send(v, v, sib))

        def hop(self, v, to):
            return send(v, v, to)

        def start(self, src=None, part_src=None):
            v = self.view(self.slot(0, 0))
            src = v if src is None else src
            self.r = send(src, v, self.right)
            self.l = send(src, v, self.left)
            self.p = send(src if part_src is None else part_src, v, self.part)
            if self.to_sib:
                self.sibs.append(send(src, v, sib))

        def near(self):
            self.r.wait_recv()
            self.fr = self.hop(self.half(self.slot(3, 0), 0), self.right)
            self.fwd(3, 0)
            self.l.wait_recv()
            self.fl = self.hop(self.half(self.slot(1, 0), 1), self.left)
            self.fwd(1, 0)

        def across(self):
            self.p.wait_recv()
            v = self.view(self.slot(0, 1))
            self.pr = self.hop(v, self.right)
            self.pl = self.hop(v, self.left)
            self.fwd(0, 1)

        def far(self):
            self.fr.wait_recv()
            self.fl.wait_recv()
            self.fwd(2, 0)

        def across_near(self):
            self.pr.wait_recv()
            self.pfr = self.hop(self.half(self.slot(3, 1), 0), self.right)
            self.fwd(3, 1)
            self.pl.wait_recv()
            self.pfl = self.hop(self.half(self.slot(1, 1), 1), self.left)
            self.fwd(1, 1)

        def across_far(self):
            self.pfr.wait_recv()
            self.pfl.wait_recv()
            self.fwd(2, 1)

        def got_sib(self, i):
            self.sibs[i].wait_recv()

    class Scatter:
        def __init__(self, view, half, slot, right, left, part, h, f, fy, fyb):
            self.view, self.half, self.slot = view, half, slot
            self.right, self.left, self.part = right, left, part
            self.h, self.f, self.fy, self.fyb = h, f, fy, fyb
            self.one, self.two = {}, {}

        def first(self, y):
            c = self.slot(2, y)
            self.one[y] = (
                send(self.half(c, 1), self.h.at[y, 0], self.right),
                send(self.half(c, 0), self.h.at[y, 1], self.left),
            )

        def second(self, y):
            for d, (dx, part, to) in enumerate(((1, 1, self.right), (3, 0, self.left))):
                self.one[y][d].wait_recv()
                v = self.half(self.slot(dx, y), part)
                v[...] = (v[...].astype(F32) + self.h.at[y, d][...].astype(F32)).astype(BF)
                copy = send(self.view(self.slot(dx, y)), self.f.at[y, d], to)
                self.two[y] = self.two.get(y, ()) + (copy,)

        def total(self, y):
            for copy in self.two[y]:
                copy.wait_recv()
            own = self.view(self.slot(0, y))
            return (
                own[...].astype(F32)
                + self.f.at[y, 0][...].astype(F32)
                + self.f.at[y, 1][...].astype(F32)
            )

        def third(self):
            self.fyb[...] = self.total(1).astype(BF)
            self.last = send(self.fyb, self.fy, self.part)

        def fourth(self):
            t = self.total(0)
            self.last.wait_recv()
            return t + self.fy[...].astype(F32)

    theirs = pl.ds(pl.multiple_of(wslot(0, 1) * WB, 128), WB)
    cols = Gather(
        lambda s: incols.at[s], lambda s, h: incols.at[s, pl.ds(160 * h, 160)],
        nslot, xr, xl, ynb, True,
    )
    cols.start(bin_hbm.at[:, mine], bin_hbm.at[:, theirs])

    put_x = []
    for to in others:
        rows = pl.ds(pl.multiple_of(to[1] * SUB, SUB), SUB)
        put_x.append(send(xv.at[rows], xw.at[w, n], to))
    xw[w, n] = xv[pl.ds(pl.multiple_of(n * SUB, SUB), SUB), :]

    load_bout.wait()

    def rotate_grad(c, _):
        at = pl.ds(pl.multiple_of(c * WB, 128), WB)
        part = jnp.dot(gv[...], bout[:, at], preferred_element_type=F32).T
        pt[0, c] = part[:NB].astype(BF)
        pt[1, c] = part[NB:].astype(BF)
        return _

    lax.fori_loop(0, 8, rotate_grad, 0)
    swap = send(pt.at[1 - k], ps, sib)

    for copy in put_x:
        copy.wait_recv()
    xg = Gather(
        lambda s: xw.at[s], lambda s, h: xw.at[s, pl.ds(8 * h, 8)], wslot, zr, zl, yq, False
    )
    xg.start()

    swap.wait_recv()
    grads = Scatter(
        lambda c: ps.at[c], lambda c, h: ps.at[c, pl.ds(160 * h, 160)],
        cslot, xr, xl, yp, rh, rf, ry, ryb,
    )

    def both(dx, dy):
        c = cslot(dx, dy)
        ps[c] = (ps[c].astype(F32) + pt[k, c].astype(F32)).astype(BF)

    both(2, 1)
    grads.first(1)
    both(2, 0)
    grads.first(0)
    for dy in (1, 0):
        for dx in (1, 3, 0):
            both(dx, dy)

    cols.near()
    xg.near()
    xg.across()
    grads.second(1)
    grads.second(0)
    cols.across()
    xg.far()
    xg.across_near()
    grads.third()
    xg.across_far()
    load_cols.wait()

    def rotate_in(dx, dy, first=False):
        total = None
        for core in range(2):
            s = cslot(dx, dy) * 2 + core
            part = jnp.dot(
                xw[:, s].reshape(8 * SUB, NB), incols[s], preferred_element_type=F32
            )
            total = part if total is None else total + part
        rotacc[...] = total if first else rotacc[...] + total

    cols.got_sib(0)
    rotate_in(0, 0, True)
    cols.far()
    rotg = grads.fourth()

    is_first = ids_ref[...] == 2 * w
    count_of = jnp.where(
        is_first, jnp.broadcast_to(cnt_ref[:, 0:1], (1, TOK)), jnp.broadcast_to(cnt_ref[:, 1:2], (1, TOK))
    )
    weight = 1.0 / count_of.astype(F32)
    gt[w, :NB] = (rotg.astype(BF).astype(F32) * weight).astype(BF)
    gt[w, NB:] = jnp.broadcast_to(jnp.where(is_first, 1.0, 0.0).astype(BF), (16, TOK))
    gg = Gather(
        lambda s: gt.at[s],
        lambda s, h: gt.at[s, pl.ds(176 * h, 176 - 16 * h)],
        wslot, zr, zl, yq, False,
    )
    gg.start()

    cols.got_sib(1)
    rotate_in(3, 0)
    cols.got_sib(2)
    rotate_in(1, 0)
    cols.across_near()
    cols.got_sib(3)
    rotate_in(0, 1)
    cols.got_sib(4)
    rotate_in(2, 0)
    gg.near()
    cols.got_sib(5)
    rotate_in(3, 1)
    cols.got_sib(6)
    rotate_in(1, 1)
    cols.across_far()
    cols.got_sib(7)
    rotate_in(2, 1)

    rot[:, pl.ds(pl.multiple_of(n * SUB, SUB), SUB), :] = (
        rotacc[...].astype(BF).reshape(8, SUB, WB)
    )

    def rows_of(s):
        return pl.ds(pl.multiple_of(s * SUB, SUB), SUB)

    rg = Gather(
        lambda s: rot.at[:, rows_of(s)],
        lambda s, h: rot.at[pl.ds(4 * h, 4), rows_of(s)],
        nslot, xr, xl, yp, True,
    )
    rg.start()
    gg.across()
    rg.near()
    rg.across()
    gg.far()
    gg.across_near()
    rg.far()
    rg.across_near()
    gg.across_far()
    rg.across_far()
    for i in range(8):
        rg.got_sib(i)

    acc[...] = jnp.zeros_like(acc)

    def fit(b, _):
        grad = gt[b, :NB]
        mask = gt[b, NB:NB + 1]
        one = grad * mask
        rows = rot[b]
        p = jnp.dot(one, rows, preferred_element_type=F32)
        r = jnp.dot(grad - one, rows, preferred_element_type=F32)
        acc[...] += p * p + r * r
        return _

    lax.fori_loop(0, 8, fit, 0)
    load_q.wait()
    eig = acc[...] * (1.0 / 16)
    acc[...] = eig
    put_eig = pltpu.make_async_copy(acc, eig_hbm, lsem.at[5])
    put_eig.start()
    scaled[...] = (qv[...].astype(F32) / (eig + damp_ref[...])).astype(BF)

    def back(s, at, wide):
        pb[s, :, pl.ds(at, wide)] = lax.dot_general(
            scaled[...], incols[pl.ds(2 * s, 2)].reshape(WB, WB)[at:at + wide],
            (((1,), (1,)), ((), ())), preferred_element_type=F32,
        ).astype(BF)

    class Part:
        def __init__(self, at, wide):
            self.at, self.wide = at, wide
            cols = pl.ds(at, wide)
            self.cols = cols
            self.es = Scatter(
                lambda s: pb.at[s, :, cols], lambda s, h: pb.at[s, pl.ds(160 * h, 160), cols],
                wslot, zr, zl, yq, eh.at[:, :, :, cols], ef.at[:, :, :, cols],
                ey.at[:, cols], eyb.at[:, cols],
            )
            self.tg = Gather(
                lambda s: tall.at[s, :, cols], lambda s, h: tall.at[s, pl.ds(160 * h, 160), cols],
                nslot, xr, xl, yp, True,
            )

        def backs(self, slots):
            for dz, dy in slots:
                back(wslot(dz, dy), self.at, self.wide)

        def begin(self):
            for y in (1, 0):
                self.backs([(2, y)])
                self.es.first(y)

        def rest(self):
            self.backs([(dz, dy) for dy in (1, 0) for dz in (1, 3, 0)])

        def gather(self):
            tall[n, :, self.cols] = self.es.fourth().astype(BF)
            self.tg.start()

        def rotate_out(self, dx, dy, i):
            self.tg.got_sib(i)
            c = cslot(dx, dy)
            rows = pl.ds(pl.multiple_of(c * WB, 128), WB)
            part = jnp.dot(
                bout[:, rows], tall[pl.ds(2 * c, 2), :, self.cols].reshape(WB, self.wide),
                preferred_element_type=F32,
            )
            out[:, self.cols] = part if i == 0 else out[:, self.cols] + part

        def near(self):
            self.rotate_out(0, 0, 0)
            self.tg.near()
            self.rotate_out(3, 0, 1)
            self.rotate_out(1, 0, 2)

        def across(self):
            self.tg.across()
            self.tg.far()
            self.rotate_out(0, 1, 3)
            self.rotate_out(2, 0, 4)

        def across_near(self):
            self.tg.across_near()
            self.rotate_out(3, 1, 5)
            self.rotate_out(1, 1, 6)

        def across_far(self):
            self.tg.across_far()
            self.rotate_out(2, 1, 7)

    a, b, c = [Part(*p) for p in PARTS]
    a.begin()
    a.rest()
    b.begin()
    b.rest()
    a.es.second(1)
    a.es.second(0)
    c.begin()
    c.rest()
    a.es.third()
    b.es.second(1)
    a.gather()
    b.es.second(0)
    c.es.second(1)
    c.es.second(0)
    b.es.third()
    a.near()
    b.gather()
    a.across()
    c.es.third()
    c.gather()
    b.near()
    a.across_near()
    b.across()
    a.across_far()
    c.near()
    b.across_near()
    c.across()
    b.across_far()
    c.across_near()
    c.across_far()
    put_out = pltpu.make_async_copy(out, out_hbm, lsem.at[6])
    put_out.start()
    put_eig.wait()
    put_out.wait()

    for copy in sent:
        copy.wait_send()


def pass_on(a_hbm, b_hbm, a_out, b_out, held, sem):
    half = NB // 2
    moves = []
    for i, (src, dst) in enumerate(((a_hbm, a_out), (b_hbm, b_out))):
        for h in range(2):
            rows = pl.ds(h * half, half)
            at = 2 * i + h
            moves.append((
                pltpu.make_async_copy(src.at[rows], held.at[at], sem.at[at, 0]),
                pltpu.make_async_copy(held.at[at], dst.at[rows], sem.at[at, 1]),
            ))
    for take, _ in moves:
        take.start()
    for take, put in moves:
        take.wait()
        put.start()
    for _, put in moves:
        put.wait()


def hand_on(a, b):
    hbm = pl.BlockSpec(memory_space=pl.ANY)
    return pl.pallas_call(
        pass_on,
        out_shape=(jax.ShapeDtypeStruct(a.shape, a.dtype), jax.ShapeDtypeStruct(b.shape, b.dtype)),
        in_specs=[hbm, hbm],
        out_specs=(hbm, hbm),
        scratch_shapes=[
            pltpu.VMEM((4, NB // 2, WB), F32), pltpu.SemaphoreType.DMA((4, 2)),
        ],
    )(a, b)


def shards(
    saved_inputs, out_grads, seq_ids, seq_counts, basis_in, basis_out, query_rotated, damping
):
    vm = pl.BlockSpec(memory_space=pltpu.VMEM)
    hbm = pl.BlockSpec(memory_space=pl.ANY)
    tile = jax.ShapeDtypeStruct((NB, WB), F32)
    tiles = pl.pallas_call(
        kernel,
        out_shape=(tile, tile),
        in_specs=[vm] * 3 + [hbm] * 5,
        out_specs=(hbm, hbm),
        scratch_shapes=[
            pltpu.VMEM((NB, TOK), BF),
            pltpu.VMEM((NB, TOK), BF),
            pltpu.VMEM((TOK, NB), BF),
            pltpu.VMEM((TOK, NB), BF),
            pltpu.VMEM((NB, WB), BF),
            pltpu.VMEM((NB, D), BF),
            pltpu.VMEM((16, NB, WB), BF),
            pltpu.VMEM((8, 16, SUB, NB), BF),
            pltpu.VMEM((2, 8, NB, TOK), BF),
            pltpu.VMEM((8, NB, TOK), BF),
            pltpu.VMEM((2, 2, NB // 2, TOK), BF),
            pltpu.VMEM((2, 2, NB, TOK), BF),
            pltpu.VMEM((NB, TOK), BF),
            pltpu.VMEM((NB, TOK), BF),
            pltpu.VMEM((8, GROWS, TOK), BF),
            pltpu.VMEM((8, TOK, WB), BF),
            pltpu.VMEM((8 * SUB, WB), F32),
            pltpu.VMEM((16, NB, WB), BF),
            pltpu.VMEM((NB, WB), F32),
            pltpu.VMEM((NB, WB), F32),
            pltpu.VMEM((NB, WB), BF),
            pltpu.VMEM((8, NB, WB), BF),
            pltpu.VMEM((2, 2, NB // 2, WB), BF),
            pltpu.VMEM((2, 2, NB, WB), BF),
            pltpu.VMEM((NB, WB), BF),
            pltpu.VMEM((NB, WB), BF),
            pltpu.SemaphoreType.DMA((NSEM,)),
            pltpu.SemaphoreType.DMA((NSEM,)),
            pltpu.SemaphoreType.DMA((7,)),
        ],
        compiler_params=pltpu.CompilerParams(
            collective_id=0, has_side_effects=True, vmem_limit_bytes=60 * 1024 * 1024
        ),
    )(
        seq_ids.reshape(1, -1), seq_counts.reshape(1, -1), damping.reshape(1, 1),
        saved_inputs.T, out_grads.T, query_rotated, basis_in, basis_out,
    )
    return hand_on(*tiles)


def solution(mesh):
    return jax.shard_map(
        shards,
        mesh=mesh,
        in_specs=(
            P("wide", "narrow"),
            P("wide", "narrow"),
            P("wide"),
            P("wide"),
            P("narrow", None),
            P("narrow", None),
            P("narrow", "wide"),
            P(),
        ),
        out_specs=(P("narrow", "wide"), P("narrow", "wide")),
        check_vma=False,
    )
```

```python
import jax
import jax.numpy as jnp
from jax import lax
from jax.experimental import pallas as pl
from jax.experimental.pallas import tpu as pltpu
from jax.sharding import PartitionSpec as P

MESH = pl.DeviceIdType.MESH
BF = jnp.bfloat16
F32 = jnp.float32

D = 5120
TOK = 256
NB = 320
WB = 640
SUB = 16
GROWS = NB + 16
PARTS = ((0, 256), (256, 256), (512, 128))
ORDER = (
    (0, 0), (1, 10), (0, 1), (1, 11), (0, 2), (1, 12), (2, 10), (0, 3), (1, 1),
    (2, 11), (2, 12), (1, 2), (0, 4), (1, 3), (0, 5), (0, 20), (2, 1), (2, 2),
    (0, 6), (0, 7), (1, 4), (0, 21), (2, 3), (2, 4), (1, 5), (0, 8), (1, 6),
    (1, 7), (1, 20), (0, 22), (2, 5), (0, 9), (2, 6), (2, 7), (1, 8), (1, 21),
    (0, 23), (2, 20), (1, 22), (2, 8), (1, 9), (2, 21), (1, 23), (2, 9), (2, 22),
    (2, 23),
)
NEAR = ((1, 1), (3, 1), (0, 1), (1, 0), (3, 0), (0, 0))
ARRIVAL = ((0, 0), (3, 0), (1, 0), (0, 1), (2, 0), (3, 1), (1, 1), (2, 1))
HALVES = ((0, 384), (384, 256))
NSEM = 384


def kernel(
    ids_ref, cnt_ref, damp_ref, x_hbm, g_hbm, q_hbm, bin_hbm, bout_hbm,
    eig_hbm, out_hbm,
    xt, gtt, xv, gv, qv, bout, incols, xw, pt, ps, rh, rf, ry, ryb, gt, rot0, rot1, rotacc, tall, acc, out,
    scaled, pb, eh, ef, ey, eyb,
    ssem, rsem, lsem,
):
    w = lax.axis_index("wide")
    n = lax.axis_index("narrow")
    yl, z = w // 4, w % 4
    yh, x, k = n // 8, (n // 2) % 4, n % 2

    def nslot(dx, dy):
        return (yh + dy) % 2 * 8 + (x + dx) % 4 * 2 + k

    def wslot(dz, dy):
        return (yl + dy) % 2 * 4 + (z + dz) % 4

    def cslot(dx, dy):
        return (yh + dy) % 2 * 4 + (x + dx) % 4

    sib = (w, n + 1 - 2 * k)
    xr, xl, yp = (w, nslot(1, 0)), (w, nslot(3, 0)), (w, nslot(0, 1))
    zr, zl, yq = (wslot(1, 0), n), (wslot(3, 0), n), (wslot(0, 1), n)
    ynb = (wslot(0, 1), nslot(0, 1))

    count = [0]
    sent = []

    def send(src, dst, to):
        c = count[0]
        count[0] += 1
        copy = pltpu.make_async_remote_copy(
            src_ref=src, dst_ref=dst, send_sem=ssem.at[c], recv_sem=rsem.at[c],
            device_id=to, device_id_type=MESH,
        )
        copy.start()
        sent.append(copy)
        return copy

    load_x = pltpu.make_async_copy(x_hbm, xt, lsem.at[2])
    load_x.start()
    load_g = pltpu.make_async_copy(g_hbm, gtt, lsem.at[3])
    load_g.start()
    load_q = pltpu.make_async_copy(q_hbm, qv, lsem.at[4])
    load_bout = pltpu.make_async_copy(bout_hbm, bout, lsem.at[0])
    load_bout.start()
    mine = pl.ds(pl.multiple_of(w * WB, 128), WB)
    load_cols = pltpu.make_async_copy(bin_hbm.at[:, mine], incols.at[n], lsem.at[1])
    load_cols.start()
    load_q.start()

    barrier = pltpu.get_barrier_semaphore()
    others = [(w, (n + d) % 16) for d in range(1, 16)]
    for to in others + [zr, zl, yq, ynb]:
        pl.semaphore_signal(barrier, inc=1, device_id=to, device_id_type=MESH)
    load_x.wait()
    xv[...] = xt[...].astype(F32).T.astype(BF)
    load_g.wait()
    gv[...] = gtt[...].astype(F32).T.astype(BF)
    pl.semaphore_wait(barrier, len(others) + 4)

    class Gather:
        def __init__(self, view, half, slot, right, left, part, to_sib, far_to=None):
            self.view, self.half, self.slot = view, half, slot
            self.right, self.left, self.part, self.to_sib = right, left, part, to_sib
            self.far_to = far_to
            self.sibs = []

        def fwd(self, dx, dy):
            if self.to_sib:
                v = self.view(self.slot(dx, dy))
                self.sibs.append(send(v, v, sib))

        def hop(self, v, to):
            return send(v, v, to)

        def start(self, src=None, part_src=None):
            v = self.view(self.slot(0, 0))
            src = v if src is None else src
            self.r = send(src, v, self.right)
            self.l = send(src, v, self.left)
            self.p = send(src if part_src is None else part_src, v, self.part)
            if self.to_sib:
                self.sibs.append(send(src, v, sib))

        def near(self):
            self.r.wait_recv()
            self.fr = self.hop(self.half(self.slot(3, 0), 0), self.right)
            self.fwd(3, 0)
            self.l.wait_recv()
            self.fl = self.hop(self.half(self.slot(1, 0), 1), self.left)
            self.fwd(1, 0)

        def across(self):
            self.p.wait_recv()
            v = self.view(self.slot(0, 1))
            self.pr = self.hop(v, self.right)
            self.pl = self.hop(v, self.left)
            self.fwd(0, 1)

        def far(self):
            self.fr.wait_recv()
            self.fl.wait_recv()
            if self.far_to is not None:
                self.pf = self.hop(self.view(self.slot(2, 0)), self.far_to)
            self.fwd(2, 0)

        def across_near(self):
            self.pr.wait_recv()
            if self.far_to is None:
                self.pfr = self.hop(self.half(self.slot(3, 1), 0), self.right)
            self.fwd(3, 1)
            self.pl.wait_recv()
            if self.far_to is None:
                self.pfl = self.hop(self.half(self.slot(1, 1), 1), self.left)
            self.fwd(1, 1)

        def across_far(self):
            if self.far_to is None:
                self.pfr.wait_recv()
                self.pfl.wait_recv()
            else:
                self.pf.wait_recv()
            self.fwd(2, 1)

        def got_sib(self, i):
            self.sibs[i].wait_recv()

    class Scatter:
        def __init__(self, view, half, slot, right, left, part, h, f, fy, fyb):
            self.view, self.half, self.slot = view, half, slot
            self.right, self.left, self.part = right, left, part
            self.h, self.f, self.fy, self.fyb = h, f, fy, fyb
            self.one, self.two = {}, {}

        def first(self, y):
            c = self.slot(2, y)
            self.one[y] = (
                send(self.half(c, 1), self.h.at[y, 0], self.right),
                send(self.half(c, 0), self.h.at[y, 1], self.left),
            )

        def second(self, y):
            for d, (dx, part, to) in enumerate(((1, 1, self.right), (3, 0, self.left))):
                self.one[y][d].wait_recv()
                v = self.half(self.slot(dx, y), part)
                v[...] = (v[...].astype(F32) + self.h.at[y, d][...].astype(F32)).astype(BF)
                copy = send(self.view(self.slot(dx, y)), self.f.at[y, d], to)
                self.two[y] = self.two.get(y, ()) + (copy,)

        def total(self, y):
            for copy in self.two[y]:
                copy.wait_recv()
            own = self.view(self.slot(0, y))
            return (
                own[...].astype(F32)
                + self.f.at[y, 0][...].astype(F32)
                + self.f.at[y, 1][...].astype(F32)
            )

        def third(self):
            self.fyb[...] = self.total(1).astype(BF)
            self.last = send(self.fyb, self.fy, self.part)

        def fourth(self):
            t = self.total(0)
            self.last.wait_recv()
            return t + self.fy[...].astype(F32)

    def rows_of(s):
        return pl.ds(pl.multiple_of(s * SUB, SUB), SUB)

    class Half:
        def __init__(self, at, wide, rot):
            self.at, self.wide, self.rot = at, wide, rot
            self.cols = cols = pl.ds(at, wide)
            self.cg = Gather(
                lambda s: incols.at[s, :, cols],
                lambda s, h: incols.at[s, pl.ds(160 * h, 160), cols],
                nslot, xr, xl, ynb, True, yp,
            )
            self.rg = Gather(
                lambda s: rot.at[:, rows_of(s)],
                lambda s, h: rot.at[pl.ds(4 * h, 4), rows_of(s)],
                nslot, xr, xl, yp, True,
            )

        def start(self):
            def of(s):
                return bin_hbm.at[:, pl.ds(pl.multiple_of(s * WB + self.at, 128), self.wide)]

            self.cg.start(of(w), of(wslot(0, 1)))

        def rotate_in(self, dx, dy, i):
            self.cg.got_sib(i)
            total = None
            for core in range(2):
                s = cslot(dx, dy) * 2 + core
                part = jnp.dot(
                    xw[:, s].reshape(8 * SUB, NB), incols[s, :, self.cols],
                    preferred_element_type=F32,
                )
                total = part if total is None else total + part
            rotacc[:, self.cols] = total if i == 0 else rotacc[:, self.cols] + total

        def spread(self):
            self.rot[:, rows_of(n)] = (
                rotacc[:, self.cols].astype(BF).reshape(8, SUB, self.wide)
            )
            self.rg.start()

        def fit(self):
            acc[:, self.cols] = jnp.zeros((NB, self.wide), F32)

            def block(b, _):
                grad = gt[b, :NB]
                mask = gt[b, NB:NB + 1]
                one = grad * mask
                rows = self.rot[b]
                p = jnp.dot(one, rows, preferred_element_type=F32)
                r = jnp.dot(grad - one, rows, preferred_element_type=F32)
                acc[:, self.cols] += p * p + r * r
                return _

            lax.fori_loop(0, 8, block, 0)

    p0, p1 = [Half(*h, rot) for h, rot in zip(HALVES, (rot0, rot1))]

    put_x = []
    for to in others:
        rows = pl.ds(pl.multiple_of(to[1] * SUB, SUB), SUB)
        put_x.append(send(xv.at[rows], xw.at[w, n], to))
    p0.start()
    xw[w, n] = xv[pl.ds(pl.multiple_of(n * SUB, SUB), SUB), :]

    load_bout.wait()

    def rotate_grad(c, _):
        at = pl.ds(pl.multiple_of(c * WB, 128), WB)
        part = jnp.dot(gv[...], bout[:, at], preferred_element_type=F32).T
        pt[0, c] = part[:NB].astype(BF)
        pt[1, c] = part[NB:].astype(BF)
        return _

    lax.fori_loop(0, 8, rotate_grad, 0)
    swap = send(pt.at[1 - k], ps, sib)

    swap.wait_recv()
    grads = Scatter(
        lambda c: ps.at[c], lambda c, h: ps.at[c, pl.ds(160 * h, 160)],
        cslot, xr, xl, yp, rh, rf, ry, ryb,
    )

    def both(dx, dy):
        c = cslot(dx, dy)
        ps[c] = (ps[c].astype(F32) + pt[k, c].astype(F32)).astype(BF)

    both(2, 1)
    grads.first(1)
    both(2, 0)
    grads.first(0)
    for dy in (1, 0):
        for dx in (1, 3, 0):
            both(dx, dy)

    for copy in put_x:
        copy.wait_recv()
    xg = Gather(
        lambda s: xw.at[s], lambda s, h: xw.at[s, pl.ds(8 * h, 8)], wslot, zr, zl, yq, False
    )
    xg.start()
    p0.cg.near()
    xg.near()
    xg.across()
    grads.second(1)
    grads.second(0)
    p0.cg.across()
    p0.cg.far()
    p1.start()
    xg.far()
    xg.across_near()
    grads.third()
    xg.across_far()
    load_cols.wait()
    p0.rotate_in(0, 0, 0)
    p0.rotate_in(3, 0, 1)
    p0.rotate_in(1, 0, 2)
    rotg = grads.fourth()

    is_first = ids_ref[...] == 2 * w
    count_of = jnp.where(
        is_first, jnp.broadcast_to(cnt_ref[:, 0:1], (1, TOK)), jnp.broadcast_to(cnt_ref[:, 1:2], (1, TOK))
    )
    weight = 1.0 / count_of.astype(F32)
    gt[w, :NB] = (rotg.astype(BF).astype(F32) * weight).astype(BF)
    gt[w, NB:] = jnp.broadcast_to(jnp.where(is_first, 1.0, 0.0).astype(BF), (16, TOK))
    gg = Gather(
        lambda s: gt.at[s],
        lambda s, h: gt.at[s, pl.ds(176 * h, 176 - 16 * h)],
        wslot, zr, zl, yq, False,
    )
    gg.start()

    p0.rotate_in(0, 1, 3)
    p0.rotate_in(2, 0, 4)
    p0.cg.across_near()
    p0.rotate_in(3, 1, 5)
    p0.rotate_in(1, 1, 6)
    p1.cg.near()
    p0.cg.across_far()
    p0.rotate_in(2, 1, 7)
    p0.spread()
    p1.cg.across()
    p1.rotate_in(0, 0, 0)
    p1.rotate_in(3, 0, 1)
    p1.rotate_in(1, 0, 2)
    p1.cg.far()
    gg.near()
    p0.rg.near()
    p1.rotate_in(0, 1, 3)
    p1.rotate_in(2, 0, 4)
    p1.cg.across_near()
    p1.rotate_in(3, 1, 5)
    p1.rotate_in(1, 1, 6)
    p0.rg.across()
    p0.rg.far()
    gg.across()
    p1.cg.across_far()
    p1.rotate_in(2, 1, 7)
    p1.spread()
    p0.rg.across_near()
    gg.far()
    gg.across_near()
    p0.rg.across_far()
    p1.rg.near()
    gg.across_far()
    p1.rg.across()
    for i in range(8):
        p0.rg.got_sib(i)
    p0.fit()
    p1.rg.far()
    p1.rg.across_near()
    p1.rg.across_far()
    for i in range(8):
        p1.rg.got_sib(i)
    p1.fit()
    load_q.wait()
    eig = acc[...] * (1.0 / 16)
    acc[...] = eig
    put_eig = pltpu.make_async_copy(acc, eig_hbm, lsem.at[5])
    put_eig.start()
    scaled[...] = (qv[...].astype(F32) / (eig + damp_ref[...])).astype(BF)

    def back(s, at, wide):
        pb[s, :, pl.ds(at, wide)] = lax.dot_general(
            scaled[...], incols[pl.ds(2 * s, 2)].reshape(WB, WB)[at:at + wide],
            (((1,), (1,)), ((), ())), preferred_element_type=F32,
        ).astype(BF)

    class Part:
        def __init__(self, at, wide):
            self.at, self.wide = at, wide
            cols = pl.ds(at, wide)
            self.cols = cols
            self.es = Scatter(
                lambda s: pb.at[s, :, cols], lambda s, h: pb.at[s, pl.ds(160 * h, 160), cols],
                wslot, zr, zl, yq, eh.at[:, :, :, cols], ef.at[:, :, :, cols],
                ey.at[:, cols], eyb.at[:, cols],
            )
            self.tg = Gather(
                lambda s: tall.at[s, :, cols], lambda s, h: tall.at[s, pl.ds(160 * h, 160), cols],
                nslot, xr, xl, yp, True,
            )

        def backs(self, slots):
            for dz, dy in slots:
                back(wslot(dz, dy), self.at, self.wide)

        def gather(self):
            tall[n, :, self.cols] = self.es.fourth().astype(BF)
            self.tg.start()

        def rotate_out(self, dx, dy, i):
            self.tg.got_sib(i)
            c = cslot(dx, dy)
            rows = pl.ds(pl.multiple_of(c * WB, 128), WB)
            part = jnp.dot(
                bout[:, rows], tall[pl.ds(2 * c, 2), :, self.cols].reshape(WB, self.wide),
                preferred_element_type=F32,
            )
            out[:, self.cols] = part if i == 0 else out[:, self.cols] + part

        def step(self, k):
            if k == 0:
                for y in (1, 0):
                    self.backs([(2, y)])
                    self.es.first(y)
                self.backs(NEAR)
            elif k == 10:
                self.backs(((2, 1), (2, 0)) + NEAR)
            elif k in (11, 12):
                self.es.first(12 - k)
            elif k in (1, 2):
                self.es.second(2 - k)
            elif k == 3:
                self.es.third()
            elif k == 4:
                self.gather()
            elif k < 10:
                (self.tg.near, self.tg.across, self.tg.far, self.tg.across_near,
                 self.tg.across_far)[k - 5]()
            else:
                for i in ((0, 1, 2), (3, 4), (5, 6), (7,))[k - 20]:
                    self.rotate_out(*ARRIVAL[i], i)

    parts = [Part(*p) for p in PARTS]
    for i, what in ORDER:
        parts[i].step(what)
    put_out = pltpu.make_async_copy(out, out_hbm, lsem.at[6])
    put_out.start()
    put_eig.wait()
    put_out.wait()

    for copy in sent:
        copy.wait_send()


def pass_on(a_hbm, b_hbm, a_out, b_out, held, sem):
    half = NB // 2
    moves = []
    for i, (src, dst) in enumerate(((a_hbm, a_out), (b_hbm, b_out))):
        for h in range(2):
            rows = pl.ds(h * half, half)
            at = 2 * i + h
            moves.append((
                pltpu.make_async_copy(src.at[rows], held.at[at], sem.at[at, 0]),
                pltpu.make_async_copy(held.at[at], dst.at[rows], sem.at[at, 1]),
            ))
    for take, _ in moves:
        take.start()
    for take, put in moves:
        take.wait()
        put.start()
    for _, put in moves:
        put.wait()


def hand_on(a, b):
    hbm = pl.BlockSpec(memory_space=pl.ANY)
    return pl.pallas_call(
        pass_on,
        out_shape=(jax.ShapeDtypeStruct(a.shape, a.dtype), jax.ShapeDtypeStruct(b.shape, b.dtype)),
        in_specs=[hbm, hbm],
        out_specs=(hbm, hbm),
        scratch_shapes=[
            pltpu.VMEM((4, NB // 2, WB), F32), pltpu.SemaphoreType.DMA((4, 2)),
        ],
    )(a, b)


def shards(
    saved_inputs, out_grads, seq_ids, seq_counts, basis_in, basis_out, query_rotated, damping
):
    vm = pl.BlockSpec(memory_space=pltpu.VMEM)
    hbm = pl.BlockSpec(memory_space=pl.ANY)
    tile = jax.ShapeDtypeStruct((NB, WB), F32)
    tiles = pl.pallas_call(
        kernel,
        out_shape=(tile, tile),
        in_specs=[vm] * 3 + [hbm] * 5,
        out_specs=(hbm, hbm),
        scratch_shapes=[
            pltpu.VMEM((NB, TOK), BF),
            pltpu.VMEM((NB, TOK), BF),
            pltpu.VMEM((TOK, NB), BF),
            pltpu.VMEM((TOK, NB), BF),
            pltpu.VMEM((NB, WB), BF),
            pltpu.VMEM((NB, D), BF),
            pltpu.VMEM((16, NB, WB), BF),
            pltpu.VMEM((8, 16, SUB, NB), BF),
            pltpu.VMEM((2, 8, NB, TOK), BF),
            pltpu.VMEM((8, NB, TOK), BF),
            pltpu.VMEM((2, 2, NB // 2, TOK), BF),
            pltpu.VMEM((2, 2, NB, TOK), BF),
            pltpu.VMEM((NB, TOK), BF),
            pltpu.VMEM((NB, TOK), BF),
            pltpu.VMEM((8, GROWS, TOK), BF),
            pltpu.VMEM((8, TOK, HALVES[0][1]), BF),
            pltpu.VMEM((8, TOK, HALVES[1][1]), BF),
            pltpu.VMEM((8 * SUB, WB), F32),
            pltpu.VMEM((16, NB, WB), BF),
            pltpu.VMEM((NB, WB), F32),
            pltpu.VMEM((NB, WB), F32),
            pltpu.VMEM((NB, WB), BF),
            pltpu.VMEM((8, NB, WB), BF),
            pltpu.VMEM((2, 2, NB // 2, WB), BF),
            pltpu.VMEM((2, 2, NB, WB), BF),
            pltpu.VMEM((NB, WB), BF),
            pltpu.VMEM((NB, WB), BF),
            pltpu.SemaphoreType.DMA((NSEM,)),
            pltpu.SemaphoreType.DMA((NSEM,)),
            pltpu.SemaphoreType.DMA((7,)),
        ],
        compiler_params=pltpu.CompilerParams(
            collective_id=0, has_side_effects=True, vmem_limit_bytes=60 * 1024 * 1024
        ),
    )(
        seq_ids.reshape(1, -1), seq_counts.reshape(1, -1), damping.reshape(1, 1),
        saved_inputs.T, out_grads.T, query_rotated, basis_in, basis_out,
    )
    return hand_on(*tiles)


def solution(mesh):
    return jax.shard_map(
        shards,
        mesh=mesh,
        in_specs=(
            P("wide", "narrow"),
            P("wide", "narrow"),
            P("wide"),
            P("wide"),
            P("narrow", None),
            P("narrow", None),
            P("narrow", "wide"),
            P(),
        ),
        out_specs=(P("narrow", "wide"), P("narrow", "wide")),
        check_vma=False,
    )
```

```python
import jax
import jax.numpy as jnp
from jax import lax
from jax.experimental import pallas as pl
from jax.experimental.pallas import tpu as pltpu
from jax.sharding import PartitionSpec as P

MESH = pl.DeviceIdType.MESH
BF = jnp.bfloat16
F32 = jnp.float32

D = 5120
TOK = 256
NB = 320
WB = 640
SUB = 16
GROWS = NB + 16
PARTS = ((0, 256), (256, 256), (512, 128))
ORDER = (
    (0, 0), (1, 10), (0, 1), (1, 11), (0, 2), (1, 12), (2, 10), (0, 3), (1, 1),
    (2, 11), (2, 12), (1, 2), (0, 4), (1, 3), (0, 5), (0, 20), (2, 1), (2, 2),
    (0, 6), (0, 7), (1, 4), (0, 21), (2, 3), (2, 4), (1, 5), (0, 8), (1, 6),
    (1, 7), (1, 20), (0, 22), (2, 5), (0, 9), (2, 6), (2, 7), (1, 8), (1, 21),
    (0, 23), (2, 20), (1, 22), (2, 8), (1, 9), (2, 21), (1, 23), (2, 9), (2, 22),
    (2, 23),
)
NEAR = ((1, 1), (3, 1), (0, 1), (1, 0), (3, 0), (0, 0))
ARRIVAL = ((0, 0), (3, 0), (1, 0), (0, 1), (2, 0), (3, 1), (1, 1), (2, 1))
HALVES = ((0, 384), (384, 256))
NSEM = 384


def kernel(
    ids_ref, cnt_ref, damp_ref, x_hbm, g_hbm, q_hbm, bin_hbm, bout_hbm,
    eig_hbm, out_hbm,
    xt, gtt, xv, gv, qv, bout, incols, xw, pt, ps, rh, rf, ry, ryb, gt, rot0, rot1, rotacc, tall, acc, out,
    scaled, pb, eh, ef, ey, eyb,
    ssem, rsem, lsem,
):
    w = lax.axis_index("wide")
    n = lax.axis_index("narrow")
    yl, z = w // 4, w % 4
    yh, x, k = n // 8, (n // 2) % 4, n % 2

    def nslot(dx, dy):
        return (yh + dy) % 2 * 8 + (x + dx) % 4 * 2 + k

    def wslot(dz, dy):
        return (yl + dy) % 2 * 4 + (z + dz) % 4

    def cslot(dx, dy):
        return (yh + dy) % 2 * 4 + (x + dx) % 4

    sib = (w, n + 1 - 2 * k)
    xr, xl, yp = (w, nslot(1, 0)), (w, nslot(3, 0)), (w, nslot(0, 1))
    zr, zl, yq = (wslot(1, 0), n), (wslot(3, 0), n), (wslot(0, 1), n)
    ynb = (wslot(0, 1), nslot(0, 1))

    count = [0]
    sent = []

    def send(src, dst, to):
        c = count[0]
        count[0] += 1
        copy = pltpu.make_async_remote_copy(
            src_ref=src, dst_ref=dst, send_sem=ssem.at[c], recv_sem=rsem.at[c],
            device_id=to, device_id_type=MESH,
        )
        copy.start()
        sent.append(copy)
        return copy

    load_x = pltpu.make_async_copy(x_hbm, xt, lsem.at[2])
    load_x.start()
    load_g = pltpu.make_async_copy(g_hbm, gtt, lsem.at[3])
    load_g.start()
    load_q = pltpu.make_async_copy(q_hbm, qv, lsem.at[4])
    load_bout = pltpu.make_async_copy(bout_hbm, bout, lsem.at[0])
    load_bout.start()
    mine = pl.ds(pl.multiple_of(w * WB, 128), WB)
    load_cols = pltpu.make_async_copy(bin_hbm.at[:, mine], incols.at[n], lsem.at[1])
    load_cols.start()
    load_q.start()

    barrier = pltpu.get_barrier_semaphore()
    others = [(w, (n + d) % 16) for d in range(1, 16)]
    for to in others + [zr, zl, yq, ynb]:
        pl.semaphore_signal(barrier, inc=1, device_id=to, device_id_type=MESH)
    load_x.wait()
    xv[...] = xt[...].astype(F32).T.astype(BF)
    load_g.wait()
    gv[...] = gtt[...].astype(F32).T.astype(BF)
    pl.semaphore_wait(barrier, len(others) + 4)

    class Gather:
        def __init__(self, view, half, slot, right, left, part, to_sib, far_to=None):
            self.view, self.half, self.slot = view, half, slot
            self.right, self.left, self.part, self.to_sib = right, left, part, to_sib
            self.far_to = far_to
            self.sibs = []

        def fwd(self, dx, dy):
            if self.to_sib:
                v = self.view(self.slot(dx, dy))
                self.sibs.append(send(v, v, sib))

        def hop(self, v, to):
            return send(v, v, to)

        def start(self, src=None, part_src=None):
            v = self.view(self.slot(0, 0))
            src = v if src is None else src
            self.r = send(src, v, self.right)
            self.l = send(src, v, self.left)
            self.p = send(src if part_src is None else part_src, v, self.part)
            if self.to_sib:
                self.sibs.append(send(src, v, sib))

        def near(self):
            self.r.wait_recv()
            self.fr = self.hop(self.half(self.slot(3, 0), 0), self.right)
            self.fwd(3, 0)
            self.l.wait_recv()
            self.fl = self.hop(self.half(self.slot(1, 0), 1), self.left)
            self.fwd(1, 0)

        def across(self):
            self.p.wait_recv()
            v = self.view(self.slot(0, 1))
            self.pr = self.hop(v, self.right)
            self.pl = self.hop(v, self.left)
            self.fwd(0, 1)

        def far(self):
            self.fr.wait_recv()
            self.fl.wait_recv()
            if self.far_to is not None:
                self.pf = self.hop(self.view(self.slot(2, 0)), self.far_to)
            self.fwd(2, 0)

        def across_near(self):
            self.pr.wait_recv()
            if self.far_to is None:
                self.pfr = self.hop(self.half(self.slot(3, 1), 0), self.right)
            self.fwd(3, 1)
            self.pl.wait_recv()
            if self.far_to is None:
                self.pfl = self.hop(self.half(self.slot(1, 1), 1), self.left)
            self.fwd(1, 1)

        def across_far(self):
            if self.far_to is None:
                self.pfr.wait_recv()
                self.pfl.wait_recv()
            else:
                self.pf.wait_recv()
            self.fwd(2, 1)

        def got_sib(self, i):
            self.sibs[i].wait_recv()

    class Scatter:
        def __init__(self, view, half, slot, right, left, part, h, f, fy, fyb):
            self.view, self.half, self.slot = view, half, slot
            self.right, self.left, self.part = right, left, part
            self.h, self.f, self.fy, self.fyb = h, f, fy, fyb
            self.one, self.two = {}, {}

        def first(self, y):
            c = self.slot(2, y)
            self.one[y] = (
                send(self.half(c, 1), self.h.at[y, 0], self.right),
                send(self.half(c, 0), self.h.at[y, 1], self.left),
            )

        def second(self, y):
            for d, (dx, part, to) in enumerate(((1, 1, self.right), (3, 0, self.left))):
                self.one[y][d].wait_recv()
                v = self.half(self.slot(dx, y), part)
                v[...] = (v[...].astype(F32) + self.h.at[y, d][...].astype(F32)).astype(BF)
                copy = send(self.view(self.slot(dx, y)), self.f.at[y, d], to)
                self.two[y] = self.two.get(y, ()) + (copy,)

        def total(self, y):
            for copy in self.two[y]:
                copy.wait_recv()
            own = self.view(self.slot(0, y))
            return (
                own[...].astype(F32)
                + self.f.at[y, 0][...].astype(F32)
                + self.f.at[y, 1][...].astype(F32)
            )

        def third(self):
            self.fyb[...] = self.total(1).astype(BF)
            self.last = send(self.fyb, self.fy, self.part)

        def fourth(self):
            t = self.total(0)
            self.last.wait_recv()
            return t + self.fy[...].astype(F32)

    def rows_of(s):
        return pl.ds(pl.multiple_of(s * SUB, SUB), SUB)

    class Half:
        def __init__(self, at, wide, rot):
            self.at, self.wide, self.rot = at, wide, rot
            self.cols = cols = pl.ds(at, wide)
            self.cg = Gather(
                lambda s: incols.at[s, :, cols],
                lambda s, h: incols.at[s, pl.ds(160 * h, 160), cols],
                nslot, xr, xl, ynb, True, yp,
            )
            self.rg = Gather(
                lambda s: rot.at[:, rows_of(s)],
                lambda s, h: rot.at[pl.ds(4 * h, 4), rows_of(s)],
                nslot, xr, xl, yp, True, yp,
            )

        def start(self):
            def of(s):
                return bin_hbm.at[:, pl.ds(pl.multiple_of(s * WB + self.at, 128), self.wide)]

            self.cg.start(of(w), of(wslot(0, 1)))

        def rotate_in(self, dx, dy, i):
            self.cg.got_sib(i)
            total = None
            for core in range(2):
                s = cslot(dx, dy) * 2 + core
                part = jnp.dot(
                    xw[:, s].reshape(8 * SUB, NB), incols[s, :, self.cols],
                    preferred_element_type=F32,
                )
                total = part if total is None else total + part
            rotacc[:, self.cols] = total if i == 0 else rotacc[:, self.cols] + total

        def spread(self):
            self.rot[:, rows_of(n)] = (
                rotacc[:, self.cols].astype(BF).reshape(8, SUB, self.wide)
            )
            self.rg.start()

        def fit(self):
            acc[:, self.cols] = jnp.zeros((NB, self.wide), F32)

            def block(b, _):
                grad = gt[b, :NB]
                mask = gt[b, NB:NB + 1]
                one = grad * mask
                rows = self.rot[b]
                p = jnp.dot(one, rows, preferred_element_type=F32)
                r = jnp.dot(grad - one, rows, preferred_element_type=F32)
                acc[:, self.cols] += p * p + r * r
                return _

            lax.fori_loop(0, 8, block, 0)

    p0, p1 = [Half(*h, rot) for h, rot in zip(HALVES, (rot0, rot1))]

    put_x = []
    for to in others:
        rows = pl.ds(pl.multiple_of(to[1] * SUB, SUB), SUB)
        put_x.append(send(xv.at[rows], xw.at[w, n], to))
    p0.start()
    xw[w, n] = xv[pl.ds(pl.multiple_of(n * SUB, SUB), SUB), :]

    load_bout.wait()

    def rotate_grad(c, _):
        at = pl.ds(pl.multiple_of(c * WB, 128), WB)
        part = jnp.dot(gv[...], bout[:, at], preferred_element_type=F32).T
        pt[0, c] = part[:NB].astype(BF)
        pt[1, c] = part[NB:].astype(BF)
        return _

    lax.fori_loop(0, 8, rotate_grad, 0)
    swap = send(pt.at[1 - k], ps, sib)

    swap.wait_recv()
    grads = Scatter(
        lambda c: ps.at[c], lambda c, h: ps.at[c, pl.ds(160 * h, 160)],
        cslot, xr, xl, yp, rh, rf, ry, ryb,
    )

    def both(dx, dy):
        c = cslot(dx, dy)
        ps[c] = (ps[c].astype(F32) + pt[k, c].astype(F32)).astype(BF)

    both(2, 1)
    grads.first(1)
    both(2, 0)
    grads.first(0)
    for dy in (1, 0):
        for dx in (1, 3, 0):
            both(dx, dy)

    for copy in put_x:
        copy.wait_recv()
    xg = Gather(
        lambda s: xw.at[s], lambda s, h: xw.at[s, pl.ds(8 * h, 8)], wslot, zr, zl, yq, False
    )
    xg.start()
    p0.cg.near()
    xg.near()
    xg.across()
    grads.second(1)
    grads.second(0)
    p0.cg.across()
    p0.cg.far()
    p1.start()
    xg.far()
    xg.across_near()
    grads.third()
    xg.across_far()
    load_cols.wait()
    p0.rotate_in(0, 0, 0)
    p0.rotate_in(3, 0, 1)
    p0.rotate_in(1, 0, 2)
    rotg = grads.fourth()

    is_first = ids_ref[...] == 2 * w
    count_of = jnp.where(
        is_first, jnp.broadcast_to(cnt_ref[:, 0:1], (1, TOK)), jnp.broadcast_to(cnt_ref[:, 1:2], (1, TOK))
    )
    weight = 1.0 / count_of.astype(F32)
    gt[w, :NB] = (rotg.astype(BF).astype(F32) * weight).astype(BF)
    gt[w, NB:] = jnp.broadcast_to(jnp.where(is_first, 1.0, 0.0).astype(BF), (16, TOK))
    gg = Gather(
        lambda s: gt.at[s],
        lambda s, h: gt.at[s, pl.ds(176 * h, 176 - 16 * h)],
        wslot, zr, zl, yq, False,
    )
    gg.start()

    p0.rotate_in(0, 1, 3)
    p0.rotate_in(2, 0, 4)
    p0.cg.across_near()
    p0.rotate_in(3, 1, 5)
    p0.rotate_in(1, 1, 6)
    p1.cg.near()
    p0.cg.across_far()
    p0.rotate_in(2, 1, 7)
    p0.spread()
    p1.cg.across()
    p1.rotate_in(0, 0, 0)
    p1.rotate_in(3, 0, 1)
    p1.rotate_in(1, 0, 2)
    p1.cg.far()
    gg.near()
    p0.rg.near()
    p1.rotate_in(0, 1, 3)
    p1.rotate_in(2, 0, 4)
    p1.cg.across_near()
    p1.rotate_in(3, 1, 5)
    p1.rotate_in(1, 1, 6)
    p0.rg.across()
    p0.rg.far()
    gg.across()
    p1.cg.across_far()
    p1.rotate_in(2, 1, 7)
    p1.spread()
    p0.rg.across_near()
    gg.far()
    gg.across_near()
    p0.rg.across_far()
    p1.rg.near()
    gg.across_far()
    p1.rg.across()
    for i in range(8):
        p0.rg.got_sib(i)
    p0.fit()
    p1.rg.far()
    p1.rg.across_near()
    p1.rg.across_far()
    for i in range(8):
        p1.rg.got_sib(i)
    p1.fit()
    load_q.wait()
    eig = acc[...] * (1.0 / 16)
    acc[...] = eig
    put_eig = pltpu.make_async_copy(acc, eig_hbm, lsem.at[5])
    put_eig.start()
    scaled[...] = (qv[...].astype(F32) / (eig + damp_ref[...])).astype(BF)

    def back(s, at, wide):
        pb[s, :, pl.ds(at, wide)] = lax.dot_general(
            scaled[...], incols[pl.ds(2 * s, 2)].reshape(WB, WB)[at:at + wide],
            (((1,), (1,)), ((), ())), preferred_element_type=F32,
        ).astype(BF)

    class Part:
        def __init__(self, at, wide):
            self.at, self.wide = at, wide
            cols = pl.ds(at, wide)
            self.cols = cols
            self.es = Scatter(
                lambda s: pb.at[s, :, cols], lambda s, h: pb.at[s, pl.ds(160 * h, 160), cols],
                wslot, zr, zl, yq, eh.at[:, :, :, cols], ef.at[:, :, :, cols],
                ey.at[:, cols], eyb.at[:, cols],
            )
            self.tg = Gather(
                lambda s: tall.at[s, :, cols], lambda s, h: tall.at[s, pl.ds(160 * h, 160), cols],
                nslot, xr, xl, yp, True,
            )

        def backs(self, slots):
            for dz, dy in slots:
                back(wslot(dz, dy), self.at, self.wide)

        def gather(self):
            tall[n, :, self.cols] = self.es.fourth().astype(BF)
            self.tg.start()

        def rotate_out(self, dx, dy, i):
            self.tg.got_sib(i)
            c = cslot(dx, dy)
            rows = pl.ds(pl.multiple_of(c * WB, 128), WB)
            part = jnp.dot(
                bout[:, rows], tall[pl.ds(2 * c, 2), :, self.cols].reshape(WB, self.wide),
                preferred_element_type=F32,
            )
            out[:, self.cols] = part if i == 0 else out[:, self.cols] + part

        def step(self, k):
            if k == 0:
                for y in (1, 0):
                    self.backs([(2, y)])
                    self.es.first(y)
                self.backs(NEAR)
            elif k == 10:
                self.backs(((2, 1), (2, 0)) + NEAR)
            elif k in (11, 12):
                self.es.first(12 - k)
            elif k in (1, 2):
                self.es.second(2 - k)
            elif k == 3:
                self.es.third()
            elif k == 4:
                self.gather()
            elif k < 10:
                (self.tg.near, self.tg.across, self.tg.far, self.tg.across_near,
                 self.tg.across_far)[k - 5]()
            else:
                for i in ((0, 1, 2), (3, 4), (5, 6), (7,))[k - 20]:
                    self.rotate_out(*ARRIVAL[i], i)

    parts = [Part(*p) for p in PARTS]
    for i, what in ORDER:
        parts[i].step(what)
    put_out = pltpu.make_async_copy(out, out_hbm, lsem.at[6])
    put_out.start()
    put_eig.wait()
    put_out.wait()

    for copy in sent:
        copy.wait_send()


def pass_on(a_hbm, b_hbm, a_out, b_out, held, sem):
    half = NB // 2
    moves = []
    for i, (src, dst) in enumerate(((a_hbm, a_out), (b_hbm, b_out))):
        for h in range(2):
            rows = pl.ds(h * half, half)
            at = 2 * i + h
            moves.append((
                pltpu.make_async_copy(src.at[rows], held.at[at], sem.at[at, 0]),
                pltpu.make_async_copy(held.at[at], dst.at[rows], sem.at[at, 1]),
            ))
    for take, _ in moves:
        take.start()
    for take, put in moves:
        take.wait()
        put.start()
    for _, put in moves:
        put.wait()


def hand_on(a, b):
    hbm = pl.BlockSpec(memory_space=pl.ANY)
    return pl.pallas_call(
        pass_on,
        out_shape=(jax.ShapeDtypeStruct(a.shape, a.dtype), jax.ShapeDtypeStruct(b.shape, b.dtype)),
        in_specs=[hbm, hbm],
        out_specs=(hbm, hbm),
        scratch_shapes=[
            pltpu.VMEM((4, NB // 2, WB), F32), pltpu.SemaphoreType.DMA((4, 2)),
        ],
    )(a, b)


def shards(
    saved_inputs, out_grads, seq_ids, seq_counts, basis_in, basis_out, query_rotated, damping
):
    vm = pl.BlockSpec(memory_space=pltpu.VMEM)
    hbm = pl.BlockSpec(memory_space=pl.ANY)
    tile = jax.ShapeDtypeStruct((NB, WB), F32)
    tiles = pl.pallas_call(
        kernel,
        out_shape=(tile, tile),
        in_specs=[vm] * 3 + [hbm] * 5,
        out_specs=(hbm, hbm),
        scratch_shapes=[
            pltpu.VMEM((NB, TOK), BF),
            pltpu.VMEM((NB, TOK), BF),
            pltpu.VMEM((TOK, NB), BF),
            pltpu.VMEM((TOK, NB), BF),
            pltpu.VMEM((NB, WB), BF),
            pltpu.VMEM((NB, D), BF),
            pltpu.VMEM((16, NB, WB), BF),
            pltpu.VMEM((8, 16, SUB, NB), BF),
            pltpu.VMEM((2, 8, NB, TOK), BF),
            pltpu.VMEM((8, NB, TOK), BF),
            pltpu.VMEM((2, 2, NB // 2, TOK), BF),
            pltpu.VMEM((2, 2, NB, TOK), BF),
            pltpu.VMEM((NB, TOK), BF),
            pltpu.VMEM((NB, TOK), BF),
            pltpu.VMEM((8, GROWS, TOK), BF),
            pltpu.VMEM((8, TOK, HALVES[0][1]), BF),
            pltpu.VMEM((8, TOK, HALVES[1][1]), BF),
            pltpu.VMEM((8 * SUB, WB), F32),
            pltpu.VMEM((16, NB, WB), BF),
            pltpu.VMEM((NB, WB), F32),
            pltpu.VMEM((NB, WB), F32),
            pltpu.VMEM((NB, WB), BF),
            pltpu.VMEM((8, NB, WB), BF),
            pltpu.VMEM((2, 2, NB // 2, WB), BF),
            pltpu.VMEM((2, 2, NB, WB), BF),
            pltpu.VMEM((NB, WB), BF),
            pltpu.VMEM((NB, WB), BF),
            pltpu.SemaphoreType.DMA((NSEM,)),
            pltpu.SemaphoreType.DMA((NSEM,)),
            pltpu.SemaphoreType.DMA((7,)),
        ],
        compiler_params=pltpu.CompilerParams(
            collective_id=0, has_side_effects=True, vmem_limit_bytes=60 * 1024 * 1024
        ),
    )(
        seq_ids.reshape(1, -1), seq_counts.reshape(1, -1), damping.reshape(1, 1),
        saved_inputs.T, out_grads.T, query_rotated, basis_in, basis_out,
    )
    return hand_on(*tiles)


def solution(mesh):
    return jax.shard_map(
        shards,
        mesh=mesh,
        in_specs=(
            P("wide", "narrow"),
            P("wide", "narrow"),
            P("wide"),
            P("wide"),
            P("narrow", None),
            P("narrow", None),
            P("narrow", "wide"),
            P(),
        ),
        out_specs=(P("narrow", "wide"), P("narrow", "wide")),
        check_vma=False,
    )
```
